32 devices in a mesh: theta: 4 (over y, core), phi: 8 (over z, x).
Axes of the slice: x: 2, y: 2, z: 4, core: 2. Of those that a mesh axis runs over, the one named last changes fastest.
Arguments:
- fields: float32 [8, 2, 1024, 4096], P(None, None, 'theta', 'phi'), may hold values from -6 to 6
- legendre: float32 [1024, 512, 1025], P('theta', 'phi'), may hold values from -0.0029296875 to 0.0029296875
- pair_table: int32 [512], replicated, may hold values from 0 to 511, each once
Outputs:
- coefficients: float32 [512, 2, 8, 1025], P(('phi', 'theta'))
The draws below stay inside these ranges and needn't reach their ends.
Inputs may be any that keep to these rules, and one draw needn't show every extreme that they name: A permutation: slot s holds the orders 1024 + pair_table[s] and 2047 - pair_table[s].
All inputs are finite; a program needn't handle non-finite values.
Results may differ from the reference program's by a relative error of at most 0.0003.
Values sent between devices are 32-bit elements; how exact they have to be, the bound alone decides.
A program may use at most 192 MiB of HBM per device.

```python
import jax
import jax.numpy as jnp
from jax import lax

LATS = 2048
HALF_LATS = 1024
LONS = 4096
DEGREES = 2048
ORDERS = 1024
LOW_ORDER = 1024
PAIRS = 512
PAIR_LEN = 1025
FIELDS = 8


def spiked(array, stream_key, source, target, shards_of, factor):
    def block_of(axis_at):
        return (jnp.arange(array.shape[axis_at]) // (array.shape[axis_at] // shards_of)).reshape((-1,) + (1,) * (array.ndim - 1 - axis_at))

    one_side = jax.random.permutation(stream_key, shards_of)[block_of(target)]
    second = (block_of(target) + shards_of // 2) % shards_of
    return jnp.where((block_of(source) == one_side) | (block_of(source) == second), factor * array, array)


def level_of(key, extent, cuts, smallest, largest):
    def one(dim, shards_of):
        draws = jax.random.uniform(jax.random.fold_in(jax.random.fold_in(key, 6), dim), (shards_of,), jnp.float32, smallest / len(cuts), largest / len(cuts))
        return jnp.repeat(jnp.exp(draws), extent[dim] // shards_of).reshape((-1,) + (1,) * (len(extent) - dim - 1))

    level = one(*cuts[0])
    for cut in cuts[1:]:
        level = level * one(*cut)
    return level


def normal_values(own_key, shape, scale, bound, cuts=(), held_as=jnp.bfloat16):
    array = jax.random.normal(own_key, shape, jnp.float32) * scale
    if len(cuts) > 0:
        array = level_of(own_key, shape, cuts, -0.22, 0.18) * array
    return jnp.clip(array, min=-bound, max=bound).astype(held_as)


def bell_draw_with(key, extent, spread, reach, shards, heavy, kind=jnp.bfloat16):
    entries = spread * jax.random.normal(key, extent, jnp.float32)
    if shards:
        entries = entries * level_of(key, extent, shards, -0.22, 0.18)
    return jnp.clip(spiked(entries, jax.random.fold_in(key, 3), *heavy), -reach, reach).astype(kind)


def setup_inputs(seed: int = 0) -> dict:
    arg_keys = jax.random.split(jax.random.key(seed), 4)
    return {
        "fields": normal_values(arg_keys[0], (FIELDS, 2, HALF_LATS, LONS), 1.0, 6.0, ((2, 4), (3, 8)), jnp.float32),
        "legendre": bell_draw_with(arg_keys[1], (HALF_LATS, PAIRS, PAIR_LEN), (LONS * LATS) ** -0.5, 0.0029296875, ((0, 4), (1, 8)), (0, 1, 8, 2.0), jnp.float32),
        "pair_table": jax.random.permutation(arg_keys[2], PAIRS).astype(jnp.int32),
    }


full_precision = lax.Precision.HIGHEST


def reference(fields, legendre, pair_table):
    spectrum = jnp.fft.rfft(fields, axis=-1)[..., LOW_ORDER:DEGREES]
    window = jnp.stack([jnp.real(spectrum), jnp.imag(spectrum)], axis=0).astype(jnp.float32)
    even = window[:, :, 0] + window[:, :, 1]
    odd = window[:, :, 0] - window[:, :, 1]
    columns = jnp.arange(PAIR_LEN, dtype=jnp.int32)

    def take(values, index):
        return lax.dynamic_index_in_dim(values, index, axis=3, keepdims=False)

    def one_slot(slot):
        pair = pair_table[slot]
        weights = lax.dynamic_index_in_dim(legendre, slot, axis=1, keepdims=False)
        first = columns < ORDERS - pair
        parity = jnp.where(first, columns % 2, (columns + pair) % 2)
        upper = ORDERS - 1 - pair

        def project(values):
            return jnp.einsum("rfj,jc->rfc", values, weights, precision=full_precision)

        even_first = project(take(even, pair))
        odd_first = project(take(odd, pair))
        even_second = project(take(even, upper))
        odd_second = project(take(odd, upper))
        lower_part = jnp.where(parity == 0, even_first, odd_first)
        upper_part = jnp.where(parity == 0, even_second, odd_second)
        return jnp.where(first, lower_part, upper_part)

    return lax.map(one_slot, jnp.arange(PAIRS, dtype=jnp.int32))
```

```python
import math

import jax
import jax.numpy as jnp
import numpy as np
from jax import lax
from jax.sharding import PartitionSpec as P

high = lax.Precision.HIGH


def add(x, y, sign=1.0):
    re = x[0] + y[0] if sign > 0 else x[0] - y[0]
    if x[1] is None and y[1] is None:
        return re, None
    if y[1] is None:
        return re, x[1]
    im = y[1] if sign > 0 else -y[1]
    return re, im if x[1] is None else x[1] + im


def turn(x, step, count):
    if step == 0:
        return x
    if 4 * step == count:
        return (x[1], -x[0]) if x[1] is not None else (jnp.zeros_like(x[0]), -x[0])
    c = float(math.cos(2 * math.pi * step / count))
    s = float(math.sin(2 * math.pi * step / count))
    if x[1] is None:
        return x[0] * c, x[0] * -s
    return x[0] * c + x[1] * s, x[1] * c - x[0] * s


def butterfly(parts):
    count = len(parts)
    if count == 1:
        return [parts[0]]
    low = butterfly(parts[0::2])
    odd = butterfly(parts[1::2])
    odd = [turn(x, i, count) for i, x in enumerate(odd)]
    return [add(x, y) for x, y in zip(low, odd)] + [add(x, y, -1.0) for x, y in zip(low, odd)]


def half_residues(parts):
    count = len(parts)
    found = butterfly([(x, None) for x in parts])
    for i in range(count // 2 + 1, count):
        re, im = found[count - i]
        found[i] = (re, -im if im is not None else None)
    return found


def on_device(fields, legendre, pair_table):
    field_count, _, lat_count, lon_count = fields.shape
    slot_count, pair_len = legendre.shape[1], legendre.shape[2]
    phi, theta = lax.axis_size("phi"), lax.axis_size("theta")
    pairs = pair_table.shape[0]
    orders = 2 * pairs
    low_order = pair_len - 1
    lons = lon_count * phi
    row_count = field_count * 2 * lat_count
    chunk = row_count // phi
    per = orders // phi

    flat = fields.reshape(phi, chunk, lon_count)
    cycles = lax.all_to_all(flat, "phi", split_axis=0, concat_axis=0, tiled=True)

    residues = half_residues([cycles[p] for p in range(phi)])
    k = np.arange(lon_count)
    rows = []
    for m0, (re, im) in enumerate(residues):
        c = jnp.asarray(np.cos(2 * np.pi * m0 * k / lons), jnp.float32)
        s = jnp.asarray(np.sin(2 * np.pi * m0 * k / lons), jnp.float32)
        if m0 == 0:
            zr, zi = re, jnp.zeros_like(re) if im is None else im
        elif im is None:
            zr, zi = re * c, -re * s
        else:
            zr, zi = re * c + im * s, im * c - re * s
        rows.append(jnp.concatenate([zr, zi], axis=1))
    stacked = jnp.concatenate(rows, axis=0)
    m1 = low_order // phi + np.arange(per)
    angles = 2 * np.pi * (np.outer(m1, k) % lon_count) / lon_count
    c, s = np.cos(angles), np.sin(angles)
    weights = jnp.asarray(np.block([[c, s], [-s, c]]), jnp.float32)
    spectra = lax.dot_general(
        weights, stacked, (((1,), (1,)), ((), ())), precision=high, preferred_element_type=jnp.float32
    ).reshape(2, orders, chunk)

    wanted = jnp.stack([pair_table, orders - 1 - pair_table], axis=1).reshape(orders)
    pick = (wanted[:, None] == jnp.arange(orders, dtype=jnp.int32)[None, :]).astype(jnp.float32)
    chosen = jnp.stack(
        [
            lax.dot_general(pick, spectra[r], (((1,), (0,)), ((), ())), precision=high,
                            preferred_element_type=jnp.float32)
            for r in range(2)
        ],
        axis=1,
    )
    grouped = lax.all_to_all(
        chosen.reshape(phi, slot_count, 2, 2, chunk), "phi", split_axis=0, concat_axis=0, tiled=True
    )
    grouped = jnp.moveaxis(grouped, 0, 3).reshape(slot_count, 2, 2, field_count, 2, lat_count)
    north, south = grouped[:, :, :, :, 0], grouped[:, :, :, :, 1]
    variants = jnp.stack([north + south, north - south], axis=1).reshape(
        slot_count, 8 * field_count, lat_count
    )
    product = lax.dot_general(
        variants, legendre, (((2,), (0,)), ((0,), (1,))), precision=high,
        preferred_element_type=jnp.float32,
    ).reshape(slot_count, 2, 2, 2, field_count, pair_len)

    own = lax.dynamic_slice_in_dim(pair_table, lax.axis_index("phi") * slot_count, slot_count)
    columns = jnp.arange(pair_len, dtype=jnp.int32)[None, :]
    shifts = own[:, None]
    first = columns < orders - shifts
    even = jnp.where(first, columns % 2, (columns + shifts) % 2) == 0
    first = first[:, None, None, :]
    even = even[:, None, None, :]
    result = jnp.where(
        first,
        jnp.where(even, product[:, 0, 0], product[:, 1, 0]),
        jnp.where(even, product[:, 0, 1], product[:, 1, 1]),
    )
    return lax.psum_scatter(result, "theta", scatter_dimension=0, tiled=True)


def solution(mesh):
    placed = (P(None, None, "theta", "phi"), P("theta", "phi", None), P())
    return jax.shard_map(
        on_device,
        mesh=mesh,
        in_specs=placed,
        out_specs=P(("phi", "theta"), None, None, None),
        check_vma=False,
    )
```
